512 devices in a mesh: box: 16 (over x, y_hi, core), sib: 2 (over y_lo), grp: 16 (over z).
Axes of the slice: x: 4, y: 4 (y_hi: 2, y_lo: 2; y = y_hi * 2 + y_lo), z: 16, core: 2. Of those that a mesh axis runs over, the one named last changes fastest.
Arguments:
- interface_maps: float32 [2, 32, 1024, 1024], P('sib', 'box', 'grp'), parts along dimension 1, may hold values from -1 to 1
- pivot_inverses: float32 [2, 32, 512, 512], P('sib', 'box', None, 'grp'), parts along dimension 1, may hold values from -1 to 5
- exterior_coupling: float32 [32, 1024, 5120], P('box', 'sib', 'grp'), parts along dimension 0, may hold values from -1 to 1
- face_blocks: int32 [32, 8], P('box'), parts along dimension 0, may hold values from 0 to 7, each once within a row
Outputs:
- interface_schur: float32 [32, 1024, 1024], P('box', 'sib', 'grp'), parts along dimension 0
- exterior_update: float32 [32, 1024, 5120], P('box', 'sib', 'grp'), parts along dimension 0
- multipliers: float32 [32, 1024, 1024], P('box', 'grp', 'sib'), parts along dimension 0
The draws below stay inside these ranges and needn't reach their ends.
There are 16 independent parts, one for each index of `box`. The reference program is written for one: setup_inputs(seed, part) draws one part's arguments, and reference() takes and returns one part's arrays. A program takes and returns all parts, laid end to end along the dimension named above; each array names one. Nothing has to cross between parts.
Inputs may be any that keep to these rules, and one draw needn't show every extreme that they name: `face_blocks`: each row is an ordering of the 8 blocks of one child: row 0 for the first child, row 1 for the second.
All inputs are finite; a program needn't handle non-finite values.
Results may differ from the reference program's by a relative error of at most 0.0001.
Values sent between devices are 32-bit elements; how exact they have to be, the bound alone decides.
A program may use at most 128 MiB of HBM per device.

```python
import math
import jax
import jax.numpy as jnp
from jax import lax

NI = 1024
PANELS = 2
NIB = 8
PW = 512
FX = 5120


def draw_pivot_inverses(key, part):
    noise_key, diagonal_key = jax.random.split(jax.random.fold_in(key, 17))
    disorder = jax.random.truncated_normal(noise_key, -6.0, 6.0, (PANELS, 2, PW, PW), jnp.float32) * (0.7 / math.sqrt(PW))
    diagonal_part = jax.random.uniform(diagonal_key, (PANELS, PW), jnp.float32, 0.5, 2.0)
    identity_block = jnp.eye(PW, dtype=jnp.float32)
    real_part = disorder[:, 0] + diagonal_part[:, :, None] * identity_block[None]
    return jnp.stack([real_part, disorder[:, 1]], axis=1)


def levels(key, extent, cuts, low, largest):
    loudness = 1.0
    for axis_at, parts in cuts:
        heights = jax.random.uniform(jax.random.fold_in(jax.random.fold_in(key, 6), axis_at), (parts,), jnp.float32, low / len(cuts), largest / len(cuts))
        loudness = loudness * jnp.repeat(jnp.exp(heights), extent[axis_at] // parts).reshape((-1,) + (1,) * (len(extent) - 1 - axis_at))
    return loudness


def centred(stream_key, shape, scale, reach, shards=(), kind=jnp.bfloat16):
    level = levels(stream_key, shape, shards, -0.22, 0.18) if shards else 1.0
    entries = jax.random.normal(stream_key, shape, jnp.float32) * scale * level
    return jnp.minimum(jnp.maximum(entries, -reach), reach).astype(kind)


def setup_inputs(seed: int = 0, part: int = 0) -> dict:
    key_of = jax.random.split(jax.random.key(seed), 5)
    own_keys = jax.random.split(jax.random.fold_in(key_of[4], part), 5)
    interface_maps = centred(own_keys[0], (2, 2, NI, NI), (2 * NI ** -0.5), 1.0, ((0, 2), (2, 16)), jnp.float32)
    pivot_inverses = draw_pivot_inverses(jax.random.fold_in(jax.random.fold_in(key_of[4], part), 71), part)
    exterior_coupling = centred(own_keys[2], (2, NI, FX), (2 * NI ** -0.5), 1.0, ((1, 2), (2, 16)), jnp.float32)
    face_blocks = jax.vmap(lambda own: jax.random.permutation(own, NIB))(jax.random.split(own_keys[3], 2)).reshape((2, NIB)).astype(jnp.int32)
    return dict(interface_maps=interface_maps, pivot_inverses=pivot_inverses, exterior_coupling=exterior_coupling, face_blocks=face_blocks)


def complex_dot(left_side, right_side):
    def product(first_part, second_part):
        return jnp.dot(first_part, second_part, precision=lax.Precision.HIGHEST, preferred_element_type=jnp.float32)

    real_part = product(left_side[0], right_side[0]) - product(left_side[1], right_side[1])
    imag_part = product(left_side[0], right_side[1]) + product(left_side[1], right_side[0])
    return jnp.stack([real_part, imag_part])


def block_sources(face_blocks):
    alpha_order = face_blocks[0].astype(jnp.int32)
    beta_order = face_blocks[1].astype(jnp.int32)
    slots = jnp.arange(face_blocks.shape[1], dtype=jnp.int32)
    beta_match = (beta_order[:, None] == slots[None, :]).astype(jnp.int32)
    alpha_match = (alpha_order[:, None] == slots[None, :]).astype(jnp.int32)
    to_beta = jnp.sum(beta_match * alpha_order[:, None], axis=0).astype(jnp.int32)
    to_alpha = jnp.sum(alpha_match * beta_order[:, None], axis=0).astype(jnp.int32)
    return to_beta, to_alpha


def reorder(matrix, source):
    blocks = source.shape[0]
    grouped = matrix.reshape(matrix.shape[0], blocks, matrix.shape[1] // blocks, matrix.shape[2])
    return jnp.take(grouped, source, axis=1).reshape(matrix.shape)


def reference(interface_maps, pivot_inverses, exterior_coupling, face_blocks):
    to_beta, to_alpha = block_sources(face_blocks)
    alpha_out = reorder(interface_maps[0], to_beta)
    beta_out = reorder(interface_maps[1], to_alpha)
    columns = []
    for panel in range(PANELS):
        section = alpha_out[:, :, panel * PW:(panel + 1) * PW]
        columns.append(complex_dot(section, pivot_inverses[panel]))
    multipliers = jnp.concatenate(columns, axis=2)
    identity_block = jnp.stack([jnp.eye(NI, dtype=jnp.float32), jnp.zeros((NI, NI), jnp.float32)])
    interface_schur = identity_block - complex_dot(multipliers, beta_out)
    exterior_update = complex_dot(multipliers, exterior_coupling)
    return interface_schur, exterior_update, multipliers
```

```python
import functools

import jax
import jax.numpy as jnp
from jax import lax
from jax.experimental import pallas as pl
from jax.experimental.pallas import tpu as pltpu
from jax.sharding import PartitionSpec as P

F32, BF16 = jnp.float32, jnp.bfloat16
NN = (((1,), (0,)), ((), ()))
NT = (((1,), (1,)), ((), ()))
R, L = 0, 1
N = 16
H = N // 2
BLOCKS = 8


def split(x):
    high = x.astype(BF16)
    return high, (x - high.astype(F32)).astype(BF16)


def dot3(a, b, dims):
    d = functools.partial(lax.dot_general, dimension_numbers=dims, preferred_element_type=F32)
    return d(a[0], b[0]) + d(a[0], b[1]) + d(a[1], b[0])


def kernel(
    tab, pt_ref, et_ref, maps_ref,
    schur_ref, ext_ref, mult_ref,
    pt_all, al_all, pack, beta, vh, vl, ph, plo, th, tl, ubuf, sbuf, rbuf,
    pss, prs, ass, ars, bss, brs, yss, yrs, uss, urs,
):
    s = lax.axis_index("sib")
    g = lax.axis_index("grp")
    other = 1 - s
    width = pt_ref.shape[2]
    fx = et_ref.shape[1]
    cols = 64
    e2 = 2 * fx
    rows = e2 + 2 * cols

    def near(d):
        return lax.rem(g + d + N, N)

    pt_all[g] = pt_ref[...]
    al_all[g] = maps_ref[:, :, 0:width]
    lane = lax.broadcasted_iota(jnp.int32, (64, 128), 1)
    for t in range(H):
        re = maps_ref[0, :, t * 128 : (t + 1) * 128]
        im = maps_ref[1, :, t * 128 : (t + 1) * 128]
        pack[2 * t] = jnp.where(lane < 64, re, pltpu.roll(im, 64, 1))
        pack[2 * t + 1] = jnp.where(lane < 64, pltpu.roll(re, 64, 1), im)

    barrier = pltpu.get_barrier_semaphore()
    for d in range(1, N):
        pl.semaphore_signal(barrier, inc=1, device_id={"grp": near(d)}, device_id_type=pl.DeviceIdType.MESH)
    pl.semaphore_signal(barrier, inc=1, device_id={"sib": other}, device_id_type=pl.DeviceIdType.MESH)
    pl.semaphore_wait(barrier, N)

    def hop(buf, ss, rs, way, k, c, arriving):
        back = k if arriving else k - 1
        shard = near(-back if way == R else back)
        return pltpu.make_async_remote_copy(
            src_ref=buf.at[shard, c], dst_ref=buf.at[shard, c],
            send_sem=ss.at[way, c, k - 1], recv_sem=rs.at[way, c, k - 1],
            device_id={"grp": near(1 if way == R else -1)}, device_id_type=pl.DeviceIdType.MESH,
        )

    def parts(k):
        for c in range(2):
            for way in (R, L):
                if k < H or way == c:
                    yield way, c

    pivot = (pt_all, pss, prs)
    alpha = (al_all, ass, ars)

    def start(ring, k):
        for way, c in parts(k):
            hop(*ring, way, k, c, False).start()

    def forward(ring, k):
        onward = tuple(parts(k))
        for way, c in parts(k - 1):
            hop(*ring, way, k - 1, c, True).wait_recv()
            if (way, c) in onward:
                hop(*ring, way, k, c, False).start()

    def arrive(ring, k):
        for way, c in parts(k):
            hop(*ring, way, k, c, True).wait_recv()

    def to_sibling(src, dst, i):
        return pltpu.make_async_remote_copy(
            src_ref=src, dst_ref=dst, send_sem=yss.at[i], recv_sem=yrs.at[i],
            device_id={"sib": other}, device_id_type=pl.DeviceIdType.MESH,
        )

    start(pivot, 1)
    alpha_over = to_sibling(maps_ref.at[:, :, pl.ds(width, width)], al_all.at[g], 0)
    beta_over = to_sibling(pack.at[:, pl.ds(0, 32), :], pack.at[:, pl.ds(0, 32), :], 1)

    @pl.when(s == 0)
    def _():
        alpha_over.start()

    @pl.when(s == 1)
    def _():
        beta_over.start()

    def prepare(c, _):
        high, low = split(et_ref[c])
        vh[pl.ds(pl.multiple_of(c * fx, 16), fx), :] = high
        vl[pl.ds(pl.multiple_of(c * fx, 16), fx), :] = low
        return 0

    lax.fori_loop(0, 2, prepare, 0)

    @pl.when(s == 0)
    def _():
        beta_over.wait_recv()

    @pl.when(s == 1)
    def _():
        alpha_over.wait_recv()

    start(alpha, 1)
    half = pl.ds(pl.multiple_of(s * 32, 32), 32)

    def push(d, arriving):
        to, source = (near(d), g) if not arriving else (g, near(-d))
        return pltpu.make_async_remote_copy(
            src_ref=pack.at[to, half, :], dst_ref=beta.at[source, half, :],
            send_sem=bss.at[d], recv_sem=brs.at[d],
            device_id={"grp": near(d)}, device_id_type=pl.DeviceIdType.MESH,
        )

    for d in range(1, N):
        push(d, False).start()
    beta[g, half, :] = pack[g, half, :]

    for ring, k in (
        (pivot, 2), (pivot, 3), (alpha, 2), (pivot, 4), (pivot, 5), (alpha, 3), (pivot, 6), (pivot, 7), (alpha, 4), (pivot, 8),
    ):
        forward(ring, k)
        if ring is pivot and k == 5:
            for d in range(1, N):
                push(d, True).wait_recv()
            to_sibling(beta.at[:, half, :], beta.at[:, half, :], 2).start()
    forward(alpha, 5)
    other_half = pl.ds(pl.multiple_of(other * 32, 32), 32)
    to_sibling(beta.at[:, other_half, :], beta.at[:, other_half, :], 2).wait_recv()
    for b in range(4):
        block = tab[9 + b]
        both = jnp.concatenate([beta[2 * block], beta[2 * block + 1]], axis=0).T
        high, low = split(both)
        vh[e2:rows, b * 128 : (b + 1) * 128] = high
        vl[e2:rows, b * 128 : (b + 1) * 128] = low
    arrive(pivot, H)

    for c in range(2):
        def widen(j, _, c=c):
            high, low = split(pt_all[j, c])
            at = pl.ds(pl.multiple_of(j * 32, 32), 32)
            ph[c, at, :] = high
            plo[c, at, :] = low
            return 0

        lax.fori_loop(0, N, widen, 0)

    def combine(z):
        a, b = z[:, 0:128], z[:, 128:256]
        return jnp.concatenate(
            [
                a[0:fx] - b[fx:e2], a[fx:e2] + b[0:fx],
                a[e2 : e2 + cols] - b[e2 + cols : rows], a[e2 + cols : rows] + b[e2 : e2 + cols],
            ],
            axis=0,
        )

    def form(q, _):
        at = pl.ds(pl.multiple_of(q * 128, 128), 128)
        right = tuple(jnp.concatenate([p[0, :, at], p[1, :, at]], axis=1) for p in (ph, plo))
        high, low = split(combine(dot3((vh[...], vl[...]), right, NN)))
        th[:, at] = high
        tl[:, at] = low
        return 0

    lax.fori_loop(0, width // 128, form, 0)

    first = lax.div(g, 2)
    sign = 1 - 2 * lax.rem(g, 2)

    def partial(i):
        block = lax.rem(first + sign * lax.div(i + 1, 2) * (1 - 2 * lax.rem(i, 2)) + BLOCKS, BLOCKS)
        right = split(
            jnp.concatenate(
                [al_all[2 * block, 0], al_all[2 * block + 1, 0], al_all[2 * block, 1], al_all[2 * block + 1, 1]], axis=0
            )
        )
        ubuf[block] = combine(dot3((th[...], tl[...]), right, NT))

    def early(i, _):
        partial(i)
        return 0

    lax.fori_loop(0, 4, early, 0)

    def slot(q):
        return pltpu.make_async_remote_copy(
            src_ref=sbuf.at[q], dst_ref=rbuf.at[q], send_sem=uss.at[q], recv_sem=urs.at[q],
            device_id={"sib": other}, device_id_type=pl.DeviceIdType.MESH,
        )

    for q in range(4):
        if q < 3:
            forward(alpha, 6 + q)
        else:
            arrive(alpha, H)
        partial(jnp.int32(4 + q))
        sbuf[q] = ubuf[tab[q]]
        slot(q).start()

    mine = tab[8]
    left = split(jnp.concatenate([al_all[mine, 0], al_all[mine, 1]], axis=0))
    zr = dot3(left, (ph[0], plo[0]), NT)
    zi = dot3(left, (ph[1], plo[1]), NT)
    mult_ref[0] = zr[0:64] - zi[64:128]
    mult_ref[1] = zi[0:64] + zr[64:128]

    for q in range(4):
        slot(q).wait_recv()
    row = lax.broadcasted_iota(jnp.int32, (cols, 128), 1) + s * 512
    col = lax.broadcasted_iota(jnp.int32, (cols, 128), 0) + g * cols
    for p in range(4):
        at = slice(p * 128, (p + 1) * 128)
        total = ubuf[tab[4 + p]] + rbuf[tab[13 + p]]
        ext_ref[0, :, at] = total[0:fx]
        ext_ref[1, :, at] = total[fx:e2]
        one = jnp.where(row + p * 128 == col, 1.0, 0.0).astype(F32)
        schur_ref[0, :, at] = one - total[e2 : e2 + cols]
        schur_ref[1, :, at] = -total[e2 + cols : rows]

    for ring in (pivot, alpha):
        for k in range(1, H + 1):
            for way, c in parts(k):
                hop(*ring, way, k, c, False).wait_send()
    for d in range(1, N):
        push(d, False).wait_send()

    @pl.when(s == 0)
    def _():
        alpha_over.wait_send()

    @pl.when(s == 1)
    def _():
        beta_over.wait_send()

    to_sibling(beta.at[:, half, :], beta.at[:, half, :], 2).wait_send()
    for q in range(4):
        slot(q).wait_send()


def tables(face_blocks, s, g):
    alpha_order, beta_order = face_blocks[0], face_blocks[1]
    slots = jnp.arange(BLOCKS, dtype=jnp.int32)
    alpha_match = (alpha_order[:, None] == slots[None, :]).astype(jnp.int32)
    beta_match = (beta_order[:, None] == slots[None, :]).astype(jnp.int32)
    to_beta = jnp.sum(beta_match * alpha_order[:, None], axis=0)
    to_alpha = jnp.sum(alpha_match * beta_order[:, None], axis=0)
    i = jnp.arange(BLOCKS, dtype=jnp.int32)
    order = (g // 2 + (1 - 2 * (g % 2)) * ((i + 1) // 2) * (1 - 2 * (i % 2)) + BLOCKS) % BLOCKS
    pick = (order[:, None] == slots[None, :]).astype(jnp.int32)
    dest = jnp.sum(pick * to_alpha[None, :], axis=1) // 4
    before = (i[:, None] > i[None, :]).astype(jnp.int32)
    leaves = (dest != s).astype(jnp.int32)
    rank_out = jnp.sum(before * leaves[None, :], axis=1)
    rank_in = jnp.sum(before * (1 - leaves)[None, :], axis=1)
    four = jnp.arange(4, dtype=jnp.int32)
    send = jnp.sum((rank_out[None, :] == four[:, None]) * leaves[None, :] * order[None, :], axis=1)
    own = lax.dynamic_slice_in_dim(to_beta, 4 * s, 4)
    arrives = jnp.sum((order[None, :] == own[:, None]) * rank_in[None, :], axis=1)
    mine = 2 * lax.dynamic_slice_in_dim(to_beta, g // 2, 1) + g % 2
    beta_blocks = lax.dynamic_slice_in_dim(to_alpha, 4 * s, 4)
    return jnp.concatenate([send, own, mine, beta_blocks, arrives]).astype(jnp.int32)


def per_device(interface_maps, pivot_inverses, exterior_coupling, face_blocks):
    s, g = lax.axis_index("sib"), lax.axis_index("grp")
    maps = interface_maps[0]
    pt = jnp.swapaxes(pivot_inverses[0], 1, 2)
    et = jnp.swapaxes(exterior_coupling, 1, 2)
    width, fx = pt.shape[2], et.shape[1]
    rows = 2 * fx + 128
    vmem = pl.BlockSpec(memory_space=pltpu.VMEM)
    dma = pltpu.SemaphoreType.DMA
    schur, ext, mult = pl.pallas_call(
        kernel,
        out_shape=(
            jax.ShapeDtypeStruct((2, 64, 512), F32),
            jax.ShapeDtypeStruct((2, fx, 512), F32),
            jax.ShapeDtypeStruct((2, 64, width), F32),
        ),
        in_specs=[pl.BlockSpec(memory_space=pltpu.SMEM)] + [vmem] * 3,
        out_specs=(vmem,) * 3,
        scratch_shapes=[
            pltpu.VMEM((N, 2, 32, width), F32),
            pltpu.VMEM((N, 2, 64, width), F32),
            pltpu.VMEM((N, 64, 128), F32),
            pltpu.VMEM((N, 64, 128), F32),
            pltpu.VMEM((rows, width), BF16),
            pltpu.VMEM((rows, width), BF16),
            pltpu.VMEM((2, width, width), BF16),
            pltpu.VMEM((2, width, width), BF16),
            pltpu.VMEM((rows, width), BF16),
            pltpu.VMEM((rows, width), BF16),
            pltpu.VMEM((BLOCKS, rows, 128), F32),
            pltpu.VMEM((4, rows, 128), F32),
            pltpu.VMEM((4, rows, 128), F32),
            dma((2, 2, H)), dma((2, 2, H)), dma((2, 2, H)), dma((2, 2, H)),
            dma((N,)), dma((N,)), dma((3,)), dma((3,)), dma((4,)), dma((4,)),
        ],
        compiler_params=pltpu.CompilerParams(collective_id=0, has_side_effects=True, vmem_limit_bytes=56 * 2**20),
    )(tables(face_blocks, s, g), pt, et, maps)
    return jnp.swapaxes(schur, 1, 2), jnp.swapaxes(ext, 1, 2), mult


def solution(mesh):
    in_specs = (P("sib", "box", "grp", None), P("sib", "box", None, "grp"), P("box", "sib", "grp"), P("box", None))
    out_specs = (P("box", "sib", "grp"), P("box", "sib", "grp"), P("box", "grp", "sib"))
    return jax.shard_map(per_device, mesh=mesh, in_specs=in_specs, out_specs=out_specs, check_vma=False)
```

```python
import functools

import jax
import jax.numpy as jnp
from jax import lax
from jax.experimental import pallas as pl
from jax.experimental.pallas import tpu as pltpu
from jax.sharding import PartitionSpec as P

F32, BF16 = jnp.float32, jnp.bfloat16
NN = (((1,), (0,)), ((), ()))
NT = (((1,), (1,)), ((), ()))
MESH = pl.DeviceIdType.MESH
R, L = 0, 1
N = 16
H = N // 2
BLOCKS = 8
COLS = 64


def split(x):
    high = x.astype(BF16)
    return high, (x - high.astype(F32)).astype(BF16)


def dot3(a, b, dims):
    d = functools.partial(lax.dot_general, dimension_numbers=dims, preferred_element_type=F32)
    return d(a[0], b[0]) + d(a[0], b[1]) + d(a[1], b[0])


def combine(z):
    half = z.shape[0] // 2
    a, b = z[:, 0:128], z[:, 128:256]
    return jnp.concatenate([a[0:half] - b[half:], a[half:] + b[0:half]], axis=0)


def look_up(keys, values, key):
    found = jnp.int32(0)
    for k, v in zip(keys, values):
        found = found + jnp.where(k == key, v, 0)
    return found


def tables(faces_ref, s, g, order):
    alpha_order = [faces_ref[0, j] for j in range(BLOCKS)]
    beta_order = [faces_ref[1, j] for j in range(BLOCKS)]
    send = [jnp.int32(0)] * 4
    out, into = jnp.int32(0), jnp.int32(0)
    rank_in = []
    for block in order:
        place = look_up(alpha_order, beta_order, block)
        leaves = jnp.where(place >= 4, 1, 0) != s
        for q in range(4):
            send[q] = send[q] + jnp.where(jnp.logical_and(leaves, out == q), block, 0)
        rank_in.append(jnp.where(leaves, 0, into))
        out = out + jnp.where(leaves, 1, 0)
        into = into + jnp.where(leaves, 0, 1)
    own = [look_up(beta_order, alpha_order, 4 * s + p) for p in range(4)]
    slots = [look_up(order, rank_in, block) for block in own]
    mine = 2 * look_up(beta_order, alpha_order, lax.div(g, 2)) + lax.rem(g, 2)
    panel = [look_up(alpha_order, beta_order, 4 * s + b) for b in range(4)]
    other_panel = [look_up(alpha_order, beta_order, 4 * (1 - s) + b) for b in range(4)]
    return send, own, slots, mine, panel, other_panel


def kernel(
    faces_ref, pt_ref, et_ref, maps_ref,
    ue_out, ub_out, re_out, rb_out, mult_ref, tab_ref,
    pt_all, al_all, pack, beta, bsend, brecv, bfull, vh, vl, bvh, bvl, ph, plo, th, tl, bth, btl, ubuf, bbuf, sbuf, sbeta,
    pss, prs, ass, ars, bss, brs, yss, yrs, uss, urs, oss,
):
    s = lax.axis_index("sib")
    g = lax.axis_index("grp")
    other = 1 - s
    width = pt_ref.shape[2]
    fx = et_ref.shape[1]

    def near(d):
        return lax.rem(g + d + N, N)

    pt_all[g] = pt_ref[...]
    al_all[g] = maps_ref[:, :, 0:width]
    lane = lax.broadcasted_iota(jnp.int32, (64, 128), 1)
    for t in range(H):
        re = maps_ref[0, :, t * 128 : (t + 1) * 128]
        im = maps_ref[1, :, t * 128 : (t + 1) * 128]
        pack[2 * t] = jnp.where(lane < 64, re, pltpu.roll(im, 64, 1))
        pack[2 * t + 1] = jnp.where(lane < 64, pltpu.roll(re, 64, 1), im)

    barrier = pltpu.get_barrier_semaphore()
    for d in range(1, N):
        pl.semaphore_signal(barrier, inc=1, device_id={"grp": near(d)}, device_id_type=MESH)
    pl.semaphore_signal(barrier, inc=1, device_id={"sib": other}, device_id_type=MESH)
    pl.semaphore_wait(barrier, N)

    def hop(buf, ss, rs, way, k, c, arriving):
        back = k if arriving else k - 1
        shard = near(-back if way == R else back)
        return pltpu.make_async_remote_copy(
            src_ref=buf.at[shard, c], dst_ref=buf.at[shard, c],
            send_sem=ss.at[way, c, k - 1], recv_sem=rs.at[way, c, k - 1],
            device_id={"grp": near(1 if way == R else -1)}, device_id_type=MESH,
        )

    def parts(k):
        for c in range(2):
            for way in (R, L):
                if k < H or way == c:
                    yield way, c

    pivot = (pt_all, pss, prs)
    alpha = (al_all, ass, ars)

    def start(ring, k):
        for way, c in parts(k):
            hop(*ring, way, k, c, False).start()

    def forward(ring, k):
        onward = tuple(parts(k))
        for way, c in parts(k - 1):
            hop(*ring, way, k - 1, c, True).wait_recv()
            if (way, c) in onward:
                hop(*ring, way, k, c, False).start()

    def arrive(ring, k):
        for way, c in parts(k):
            hop(*ring, way, k, c, True).wait_recv()

    def to_sibling(src, dst, send_sem, recv_sem):
        return pltpu.make_async_remote_copy(
            src_ref=src, dst_ref=dst, send_sem=send_sem, recv_sem=recv_sem, device_id={"sib": other}, device_id_type=MESH
        )

    start(pivot, 1)
    alpha_over = to_sibling(maps_ref.at[:, :, pl.ds(width, width)], al_all.at[g], yss.at[0], yrs.at[0])
    beta_over = to_sibling(pack.at[:, pl.ds(0, 32), :], pack.at[:, pl.ds(0, 32), :], yss.at[1], yrs.at[1])
    panel_over = to_sibling(bsend, brecv, yss.at[2], yrs.at[2])
    rest_over = to_sibling(sbeta, rb_out, yss.at[3], yrs.at[3])

    @pl.when(s == 0)
    def _():
        alpha_over.start()
        start(alpha, 1)

    @pl.when(s == 1)
    def _():
        beta_over.start()

    def prepare(c, _):
        at = pl.ds(pl.multiple_of(c * fx, 16), fx)
        high, low = split(et_ref[c])
        vh[at, :] = high
        vl[at, :] = low
        return 0

    lax.fori_loop(0, 2, prepare, 0)

    first = lax.div(g, 2)
    sign = 1 - 2 * lax.rem(g, 2)

    def completes(i):
        return lax.rem(first + sign * lax.div(i + 1, 2) * (1 - 2 * lax.rem(i, 2)) + BLOCKS, BLOCKS)

    forward(pivot, 2)
    send, own, slots, mine, panel, other_panel = tables(faces_ref, s, g, [completes(jnp.int32(i)) for i in range(BLOCKS)])
    for p in range(4):
        tab_ref[p] = own[p]
        tab_ref[4 + p] = slots[p]

    @pl.when(s == 0)
    def _():
        beta_over.wait_recv()

    @pl.when(s == 1)
    def _():
        alpha_over.wait_recv()
        start(alpha, 1)

    half = pl.ds(pl.multiple_of(s * 32, 32), 32)

    def push(d, arriving):
        to, source = (near(d), g) if not arriving else (g, near(-d))
        return pltpu.make_async_remote_copy(
            src_ref=pack.at[to, half, :], dst_ref=beta.at[source, half, :],
            send_sem=bss.at[d], recv_sem=brs.at[d],
            device_id={"grp": near(d)}, device_id_type=MESH,
        )

    for ring, k in ((pivot, 3), (pivot, 4), (alpha, 2), (pivot, 5), (pivot, 6), (pivot, 7), (pivot, 8), (alpha, 3)):
        forward(ring, k)
    arrive(pivot, H)

    for c in range(2):
        def widen(j, _, c=c):
            high, low = split(pt_all[j, c])
            at = pl.ds(pl.multiple_of(j * 32, 32), 32)
            ph[c, at, :] = high
            plo[c, at, :] = low
            return 0

        lax.fori_loop(0, N, widen, 0)

    def form(q, left, high_ref, low_ref):
        at = pl.ds(pl.multiple_of(q * 128, 128), 128)
        right = tuple(jnp.concatenate([p[0, :, at], p[1, :, at]], axis=1) for p in (ph, plo))
        high, low = split(combine(dot3(tuple(ref[...] for ref in left), right, NN)))
        high_ref[:, at] = high
        low_ref[:, at] = low

    def form_exterior(q, _):
        form(q, (vh, vl), th, tl)
        return 0

    def form_beta(q, _):
        form(q, (bvh, bvl), bth, btl)
        return 0

    def rows_of(block):
        a, b = al_all.at[2 * block], al_all.at[2 * block + 1]
        return split(jnp.concatenate([a[0], b[0], a[1], b[1]], axis=0))

    def keep(block):
        return pltpu.make_async_copy(ubuf.at[block], ue_out.at[block], oss.at[block])

    def partial(i, _):
        block = completes(i)
        ubuf[block] = combine(dot3((th[...], tl[...]), rows_of(block), NT))
        keep(block).start()
        return 0

    def partial_beta(block, _):
        bbuf[block] = combine(dot3((bth[...], btl[...]), rows_of(block), NT))
        return 0

    def slot(q):
        return to_sibling(sbuf.at[q], re_out.at[q], uss.at[q], urs.at[q])

    def ship(q):
        partial(jnp.int32(4 + q), 0)
        sbuf[q] = ubuf[send[q]]
        slot(q).start()

    lax.fori_loop(0, 2, form_exterior, 0)
    forward(alpha, 4)
    lax.fori_loop(2, 4, form_exterior, 0)
    forward(alpha, 5)
    lax.fori_loop(0, 4, partial, 0)
    forward(alpha, 6)
    ship(0)
    forward(alpha, 7)
    for d in range(1, N):
        push(d, False).start()
    beta[g, half, :] = pack[g, half, :]
    ship(1)
    forward(alpha, 8)
    ship(2)

    for d in range(1, N):
        push(d, True).wait_recv()
    for b in range(4):
        for c in range(2):
            bsend[b, c] = beta[2 * other_panel[b] + c, half, :]
    panel_over.start()
    arrive(alpha, H)
    ship(3)

    panel_over.wait_recv()
    for b in range(4):
        for c in range(2):
            bfull[c, half, :] = beta[2 * panel[b] + c, half, :]
            bfull[c, pl.ds(pl.multiple_of(other * 32, 32), 32), :] = brecv[b, c]
        high, low = split(bfull[...].reshape(128, 128).T)
        bvh[:, b * 128 : (b + 1) * 128] = high
        bvl[:, b * 128 : (b + 1) * 128] = low
    lax.fori_loop(0, 4, form_beta, 0)
    lax.fori_loop(0, BLOCKS, partial_beta, 0)
    for q in range(4):
        sbeta[q] = bbuf[send[q]]
    rest_over.start()
    keep_beta = pltpu.make_async_copy(bbuf, ub_out, oss.at[BLOCKS])
    keep_beta.start()

    left = split(jnp.concatenate([al_all[mine, 0], al_all[mine, 1]], axis=0))
    zr = dot3(left, (ph[0], plo[0]), NT)
    zi = dot3(left, (ph[1], plo[1]), NT)
    mult_ref[0] = zr[0:64] - zi[64:128]
    mult_ref[1] = zi[0:64] + zr[64:128]

    for ring in (pivot, alpha):
        for k in range(1, H + 1):
            for way, c in parts(k):
                hop(*ring, way, k, c, False).wait_send()
    for d in range(1, N):
        push(d, False).wait_send()

    @pl.when(s == 0)
    def _():
        alpha_over.wait_send()

    @pl.when(s == 1)
    def _():
        beta_over.wait_send()

    for block in range(BLOCKS):
        keep(block).wait()
    keep_beta.wait()
    panel_over.wait_send()
    for q in range(4):
        slot(q).wait()
    rest_over.wait()


def place(tab, ue_ref, ub_ref, re_ref, rb_ref, mult_ref, schur_ref, ext_ref, out_ref):
    p = pl.program_id(0)
    fx = ext_ref.shape[1]
    ext_ref[0] = ue_ref[0, 0:fx] + re_ref[0, 0:fx]
    ext_ref[1] = ue_ref[0, fx:] + re_ref[0, fx:]
    row = lax.broadcasted_iota(jnp.int32, (COLS, 128), 1) + (lax.axis_index("sib") * 4 + p) * 128
    col = lax.broadcasted_iota(jnp.int32, (COLS, 128), 0) + lax.axis_index("grp") * COLS
    one = jnp.where(row == col, 1.0, 0.0).astype(F32)
    schur_ref[0] = one - (ub_ref[0, 0:COLS] + rb_ref[0, 0:COLS])
    schur_ref[1] = -(ub_ref[0, COLS:] + rb_ref[0, COLS:])
    out_ref[...] = mult_ref[...]


def per_device(interface_maps, pivot_inverses, exterior_coupling, face_blocks):
    maps = interface_maps[0]
    pt = jnp.swapaxes(pivot_inverses[0], 1, 2)
    et = jnp.swapaxes(exterior_coupling, 1, 2)
    width, fx = pt.shape[2], et.shape[1]
    vmem = pl.BlockSpec(memory_space=pltpu.VMEM)
    smem = pl.BlockSpec(memory_space=pltpu.SMEM)
    hbm = pl.BlockSpec(memory_space=pltpu.HBM)
    dma = pltpu.SemaphoreType.DMA
    ue, ub, re, rb, mult, tab = pl.pallas_call(
        kernel,
        out_shape=(
            jax.ShapeDtypeStruct((BLOCKS, 2 * fx, 128), F32),
            jax.ShapeDtypeStruct((BLOCKS, 2 * COLS, 128), F32),
            jax.ShapeDtypeStruct((4, 2 * fx, 128), F32),
            jax.ShapeDtypeStruct((4, 2 * COLS, 128), F32),
            jax.ShapeDtypeStruct((2, 64, width), F32),
            jax.ShapeDtypeStruct((8,), jnp.int32),
        ),
        in_specs=[smem, vmem, vmem, vmem],
        out_specs=(hbm, hbm, hbm, hbm, vmem, smem),
        scratch_shapes=[
            pltpu.VMEM((N, 2, 32, width), F32),
            pltpu.VMEM((N, 2, 64, width), F32),
            pltpu.VMEM((N, 64, 128), F32),
            pltpu.VMEM((N, 64, 128), F32),
            pltpu.VMEM((4, 2, 32, 128), F32),
            pltpu.VMEM((4, 2, 32, 128), F32),
            pltpu.VMEM((2, 64, 128), F32),
            pltpu.VMEM((2 * fx, width), BF16),
            pltpu.VMEM((2 * fx, width), BF16),
            pltpu.VMEM((2 * COLS, width), BF16),
            pltpu.VMEM((2 * COLS, width), BF16),
            pltpu.VMEM((2, width, width), BF16),
            pltpu.VMEM((2, width, width), BF16),
            pltpu.VMEM((2 * fx, width), BF16),
            pltpu.VMEM((2 * fx, width), BF16),
            pltpu.VMEM((2 * COLS, width), BF16),
            pltpu.VMEM((2 * COLS, width), BF16),
            pltpu.VMEM((BLOCKS, 2 * fx, 128), F32),
            pltpu.VMEM((BLOCKS, 2 * COLS, 128), F32),
            pltpu.VMEM((4, 2 * fx, 128), F32),
            pltpu.VMEM((4, 2 * COLS, 128), F32),
            dma((2, 2, H)), dma((2, 2, H)), dma((2, 2, H)), dma((2, 2, H)),
            dma((N,)), dma((N,)), dma((4,)), dma((4,)), dma((4,)), dma((4,)), dma((BLOCKS + 1,)),
        ],
        compiler_params=pltpu.CompilerParams(collective_id=0, has_side_effects=True, vmem_limit_bytes=56 * 2**20),
    )(face_blocks, pt, et, maps)

    def block(shape, index):
        return pl.BlockSpec(shape, index)

    schur, ext, mult = pl.pallas_call(
        place,
        grid_spec=pltpu.PrefetchScalarGridSpec(
            num_scalar_prefetch=1,
            grid=(4,),
            in_specs=[
                block((1, 2 * fx, 128), lambda p, tab: (tab[p], 0, 0)),
                block((1, 2 * COLS, 128), lambda p, tab: (tab[p], 0, 0)),
                block((1, 2 * fx, 128), lambda p, tab: (tab[4 + p], 0, 0)),
                block((1, 2 * COLS, 128), lambda p, tab: (tab[4 + p], 0, 0)),
                block((2, 64, 128), lambda p, tab: (0, 0, p)),
            ],
            out_specs=[
                block((2, COLS, 128), lambda p, tab: (0, 0, p)),
                block((2, fx, 128), lambda p, tab: (0, 0, p)),
                block((2, 64, 128), lambda p, tab: (0, 0, p)),
            ],
        ),
        out_shape=(
            jax.ShapeDtypeStruct((2, COLS, 512), F32),
            jax.ShapeDtypeStruct((2, fx, 512), F32),
            jax.ShapeDtypeStruct((2, 64, width), F32),
        ),
    )(tab, ue, ub, re, rb, mult)
    return jnp.swapaxes(schur, 1, 2), jnp.swapaxes(ext, 1, 2), mult


def solution(mesh):
    in_specs = (P("sib", "box", "grp", None), P("sib", "box", None, "grp"), P("box", "sib", "grp"), P("box", None))
    out_specs = (P("box", "sib", "grp"), P("box", "sib", "grp"), P("box", "grp", "sib"))
    return jax.shard_map(per_device, mesh=mesh, in_specs=in_specs, out_specs=out_specs, check_vma=False)
```

```python
import functools

import jax
import jax.numpy as jnp
from jax import lax
from jax.experimental import pallas as pl
from jax.experimental.pallas import tpu as pltpu
from jax.sharding import PartitionSpec as P

F32, BF16 = jnp.float32, jnp.bfloat16
NN = (((1,), (0,)), ((), ()))
NT = (((1,), (1,)), ((), ()))
MESH = pl.DeviceIdType.MESH
R, L = 0, 1
N = 16
H = N // 2
BLOCKS = 8
COLS = 64


def split(x):
    high = x.astype(BF16)
    return high, (x - high.astype(F32)).astype(BF16)


def dot3(a, b, dims):
    d = functools.partial(lax.dot_general, dimension_numbers=dims, preferred_element_type=F32)
    return d(a[0], b[0]) + d(a[0], b[1]) + d(a[1], b[0])


def combine(z):
    half = z.shape[0] // 2
    a, b = z[:, 0:128], z[:, 128:256]
    return jnp.concatenate([a[0:half] - b[half:], a[half:] + b[0:half]], axis=0)


def look_up(keys, values, key):
    found = jnp.int32(0)
    for k, v in zip(keys, values):
        found = found + jnp.where(k == key, v, 0)
    return found


def tables(faces_ref, s, g, order):
    alpha_order = [faces_ref[0, j] for j in range(BLOCKS)]
    beta_order = [faces_ref[1, j] for j in range(BLOCKS)]
    send = [jnp.int32(0)] * 4
    out, into = jnp.int32(0), jnp.int32(0)
    rank_in = []
    for block in order:
        place = look_up(alpha_order, beta_order, block)
        leaves = jnp.where(place >= 4, 1, 0) != s
        for q in range(4):
            send[q] = send[q] + jnp.where(jnp.logical_and(leaves, out == q), block, 0)
        rank_in.append(jnp.where(leaves, 0, into))
        out = out + jnp.where(leaves, 1, 0)
        into = into + jnp.where(leaves, 0, 1)
    own = [look_up(beta_order, alpha_order, 4 * s + p) for p in range(4)]
    slots = [look_up(order, rank_in, block) for block in own]
    mine = 2 * look_up(beta_order, alpha_order, lax.div(g, 2)) + lax.rem(g, 2)
    panel = [look_up(alpha_order, beta_order, 4 * s + b) for b in range(4)]
    other_panel = [look_up(alpha_order, beta_order, 4 * (1 - s) + b) for b in range(4)]
    return send, own, slots, mine, panel, other_panel


def kernel(
    faces_ref, pt_ref, et_ref, maps_ref,
    ue_out, ub_out, re_out, rb_out, mult_ref, tab_ref,
    pt_all, al_all, pack, held, et_in, beta, bsend, brecv, bfull, vh, vl, bvh, bvl, ph, plo, th, tl, bth, btl, ubuf, bbuf, sbuf, sbeta,
    pss, prs, ass, ars, bss, brs, yss, yrs, uss, urs, oss, ess,
):
    s = lax.axis_index("sib")
    g = lax.axis_index("grp")
    other = 1 - s
    width = pt_ref.shape[2]
    fx = et_ref.shape[1]
    width2 = pl.ds(width, width)

    def near(d):
        return lax.rem(g + d + N, N)

    barrier = pltpu.get_barrier_semaphore()
    for peer in ({"grp": near(1)}, {"grp": near(-1)}, {"sib": other}):
        pl.semaphore_signal(barrier, inc=1, device_id=peer, device_id_type=MESH)
    fetch = pltpu.make_async_copy(et_ref, et_in, ess)
    fetch.start()

    pt_all[g] = pt_ref[...]

    @pl.when(s == 0)
    def _():
        al_all[g] = maps_ref[:, :, 0:width]

    @pl.when(s == 1)
    def _():
        lane = lax.broadcasted_iota(jnp.int32, (32, 128), 1)
        for ref, at in ((pack, 0), (held, 32)):
            for t in range(H):
                re = maps_ref[0, at : at + 32, t * 128 : (t + 1) * 128]
                im = maps_ref[1, at : at + 32, t * 128 : (t + 1) * 128]
                ref[2 * t] = jnp.where(lane < 64, re, pltpu.roll(im, 64, 1))
                ref[2 * t + 1] = jnp.where(lane < 64, pltpu.roll(re, 64, 1), im)

    pl.semaphore_wait(barrier, 3)

    def hop(buf, ss, rs, way, k, c, arriving):
        back = k if arriving else k - 1
        shard = near(-back if way == R else back)
        return pltpu.make_async_remote_copy(
            src_ref=buf.at[shard, c], dst_ref=buf.at[shard, c],
            send_sem=ss.at[way, c, k - 1], recv_sem=rs.at[way, c, k - 1],
            device_id={"grp": near(1 if way == R else -1)}, device_id_type=MESH,
        )

    def parts(k):
        for c in range(2):
            for way in (R, L):
                if k < H or way == c:
                    yield way, c

    pivot = (pt_all, pss, prs)
    alpha = (al_all, ass, ars)

    def start(ring, k):
        for way, c in parts(k):
            hop(*ring, way, k, c, False).start()

    def forward(ring, k):
        onward = tuple(parts(k))
        for way, c in parts(k - 1):
            hop(*ring, way, k - 1, c, True).wait_recv()
            if (way, c) in onward:
                hop(*ring, way, k, c, False).start()

    def arrive(ring, k):
        for way, c in parts(k):
            hop(*ring, way, k, c, True).wait_recv()

    def to_sibling(src, dst, send_sem, recv_sem):
        return pltpu.make_async_remote_copy(
            src_ref=src, dst_ref=dst, send_sem=send_sem, recv_sem=recv_sem, device_id={"sib": other}, device_id_type=MESH
        )

    start(pivot, 1)
    alpha_over = [to_sibling(maps_ref.at[c, :, width2], al_all.at[g, c], yss.at[4 + c], yrs.at[4 + c]) for c in range(2)]
    beta_over = to_sibling(pack, held, yss.at[1], yrs.at[1])
    panel_over = to_sibling(bsend, brecv, yss.at[2], yrs.at[2])
    rest_over = to_sibling(sbeta, rb_out, yss.at[3], yrs.at[3])

    @pl.when(s == 0)
    def _():
        for copy in alpha_over:
            copy.start()
        start(alpha, 1)

    @pl.when(s == 1)
    def _():
        beta_over.start()

    forward(pivot, 2)

    @pl.when(s == 1)
    def _():
        for c in range(2):
            alpha_over[c].wait_recv()
            for way in (R, L):
                hop(*alpha, way, 1, c, False).start()

    fetch.wait()

    def prepare(c, _):
        at = pl.ds(pl.multiple_of(c * fx, 16), fx)
        high, low = split(et_in[c])
        vh[at, :] = high
        vl[at, :] = low
        return 0

    lax.fori_loop(0, 2, prepare, 0)

    first = lax.div(g, 2)
    sign = 1 - 2 * lax.rem(g, 2)

    def completes(i):
        return lax.rem(first + sign * lax.div(i + 1, 2) * (1 - 2 * lax.rem(i, 2)) + BLOCKS, BLOCKS)

    forward(pivot, 3)
    send, own, slots, mine, panel, other_panel = tables(faces_ref, s, g, [completes(jnp.int32(i)) for i in range(BLOCKS)])
    for p in range(4):
        tab_ref[p] = own[p]
        tab_ref[4 + p] = slots[p]

    half = pl.ds(pl.multiple_of(s * 32, 32), 32)

    def push(d, arriving):
        to, source = (near(d), g) if not arriving else (g, near(-d))
        return pltpu.make_async_remote_copy(
            src_ref=held.at[to], dst_ref=beta.at[source, half, :],
            send_sem=bss.at[d], recv_sem=brs.at[d],
            device_id={"grp": near(d)}, device_id_type=MESH,
        )

    for ring, k in ((pivot, 4), (alpha, 2), (pivot, 5), (pivot, 6), (alpha, 3), (pivot, 7), (pivot, 8), (alpha, 4)):
        forward(ring, k)
    arrive(pivot, H)

    for c in range(2):
        def widen(j, _, c=c):
            high, low = split(pt_all[j, c])
            at = pl.ds(pl.multiple_of(j * 32, 32), 32)
            ph[c, at, :] = high
            plo[c, at, :] = low
            return 0

        lax.fori_loop(0, N, widen, 0)

    def form(q, left, high_ref, low_ref):
        at = pl.ds(pl.multiple_of(q * 128, 128), 128)
        right = tuple(jnp.concatenate([p[0, :, at], p[1, :, at]], axis=1) for p in (ph, plo))
        high, low = split(combine(dot3(tuple(ref[...] for ref in left), right, NN)))
        high_ref[:, at] = high
        low_ref[:, at] = low

    def form_exterior(q, _):
        form(q, (vh, vl), th, tl)
        return 0

    def form_beta(q, _):
        form(q, (bvh, bvl), bth, btl)
        return 0

    def rows_of(block):
        a, b = al_all.at[2 * block], al_all.at[2 * block + 1]
        return split(jnp.concatenate([a[0], b[0], a[1], b[1]], axis=0))

    def keep(block):
        return pltpu.make_async_copy(ubuf.at[block], ue_out.at[block], oss.at[block])

    def partial(i, _):
        block = completes(i)
        ubuf[block] = combine(dot3((th[...], tl[...]), rows_of(block), NT))
        keep(block).start()
        return 0

    def partial_beta(block, _):
        bbuf[block] = combine(dot3((bth[...], btl[...]), rows_of(block), NT))
        return 0

    def slot(q):
        return to_sibling(sbuf.at[q], re_out.at[q], uss.at[q], urs.at[q])

    def ship(q):
        partial(jnp.int32(4 + q), 0)
        sbuf[q] = ubuf[send[q]]
        slot(q).start()

    lax.fori_loop(0, 4, form_exterior, 0)
    forward(alpha, 5)
    lax.fori_loop(0, 4, partial, 0)
    forward(alpha, 6)
    ship(0)
    forward(alpha, 7)

    @pl.when(s == 0)
    def _():
        beta_over.wait_recv()

    for d in range(1, N):
        push(d, False).start()
    beta[g, half, :] = held[g]
    ship(1)
    forward(alpha, 8)
    ship(2)

    for d in range(1, N):
        push(d, True).wait_recv()
    for b in range(4):
        for c in range(2):
            bsend[b, c] = beta[2 * other_panel[b] + c, half, :]
    panel_over.start()
    arrive(alpha, H)
    ship(3)

    panel_over.wait_recv()
    for b in range(4):
        for c in range(2):
            bfull[c, half, :] = beta[2 * panel[b] + c, half, :]
            bfull[c, pl.ds(pl.multiple_of(other * 32, 32), 32), :] = brecv[b, c]
        high, low = split(bfull[...].reshape(128, 128).T)
        bvh[:, b * 128 : (b + 1) * 128] = high
        bvl[:, b * 128 : (b + 1) * 128] = low
    lax.fori_loop(0, 4, form_beta, 0)
    lax.fori_loop(0, BLOCKS, partial_beta, 0)
    for q in range(4):
        sbeta[q] = bbuf[send[q]]
    rest_over.start()
    keep_beta = pltpu.make_async_copy(bbuf, ub_out, oss.at[BLOCKS])
    keep_beta.start()

    left = split(jnp.concatenate([al_all[mine, 0], al_all[mine, 1]], axis=0))
    zr = dot3(left, (ph[0], plo[0]), NT)
    zi = dot3(left, (ph[1], plo[1]), NT)
    mult_ref[0] = zr[0:64] - zi[64:128]
    mult_ref[1] = zi[0:64] + zr[64:128]

    for ring in (pivot, alpha):
        for k in range(1, H + 1):
            for way, c in parts(k):
                hop(*ring, way, k, c, False).wait_send()
    for d in range(1, N):
        push(d, False).wait_send()

    @pl.when(s == 0)
    def _():
        for copy in alpha_over:
            copy.wait_send()

    @pl.when(s == 1)
    def _():
        beta_over.wait_send()

    for block in range(BLOCKS):
        keep(block).wait()
    keep_beta.wait()
    panel_over.wait_send()
    for q in range(4):
        slot(q).wait()
    rest_over.wait()


def place(tab, ue_ref, ub_ref, re_ref, rb_ref, mult_ref, schur_ref, ext_ref, out_ref, ue, ub, re, rb, mult, schur, ext, sems):
    fx = ext_ref.shape[1]
    through = pltpu.make_async_copy(mult_ref, mult, sems.at[0, 8])
    through.start()
    reads, writes = [], []
    for p in range(4):
        own, slot = tab[p], tab[4 + p]
        pairs = ((ue_ref.at[own], ue.at[p]), (re_ref.at[slot], re.at[p]), (ub_ref.at[own], ub.at[p]), (rb_ref.at[slot], rb.at[p]))
        reads.append([pltpu.make_async_copy(a, b, sems.at[p, i]) for i, (a, b) in enumerate(pairs)])
        for copy in reads[p]:
            copy.start()
    col = lax.broadcasted_iota(jnp.int32, (COLS, 128), 0) + lax.axis_index("grp") * COLS
    row = lax.broadcasted_iota(jnp.int32, (COLS, 128), 1) + lax.axis_index("sib") * 512
    for p in range(4):
        at = slice(p * 128, (p + 1) * 128)
        for copy in reads[p]:
            copy.wait()
        ext[0, :, at] = ue[p, 0:fx] + re[p, 0:fx]
        ext[1, :, at] = ue[p, fx:] + re[p, fx:]
        one = jnp.where(row + p * 128 == col, 1.0, 0.0).astype(F32)
        schur[0, :, at] = one - (ub[p, 0:COLS] + rb[p, 0:COLS])
        schur[1, :, at] = -(ub[p, COLS:] + rb[p, COLS:])
        for i, (a, b) in enumerate(((ext, ext_ref), (schur, schur_ref))):
            writes.append(pltpu.make_async_copy(a.at[:, :, at], b.at[:, :, at], sems.at[p, 4 + i]))
            writes[-1].start()
    through.wait()
    writes.append(pltpu.make_async_copy(mult, out_ref, sems.at[1, 8]))
    writes[-1].start()
    for copy in writes:
        copy.wait()


def per_device(interface_maps, pivot_inverses, exterior_coupling, face_blocks):
    maps = interface_maps[0]
    pt = jnp.swapaxes(pivot_inverses[0], 1, 2)
    et = jnp.swapaxes(exterior_coupling, 1, 2)
    width, fx = pt.shape[2], et.shape[1]
    vmem = pl.BlockSpec(memory_space=pltpu.VMEM)
    smem = pl.BlockSpec(memory_space=pltpu.SMEM)
    hbm = pl.BlockSpec(memory_space=pltpu.HBM)
    dma = pltpu.SemaphoreType.DMA
    ue, ub, re, rb, mult, tab = pl.pallas_call(
        kernel,
        out_shape=(
            jax.ShapeDtypeStruct((BLOCKS, 2 * fx, 128), F32),
            jax.ShapeDtypeStruct((BLOCKS, 2 * COLS, 128), F32),
            jax.ShapeDtypeStruct((4, 2 * fx, 128), F32),
            jax.ShapeDtypeStruct((4, 2 * COLS, 128), F32),
            jax.ShapeDtypeStruct((2, 64, width), F32),
            jax.ShapeDtypeStruct((8,), jnp.int32),
        ),
        in_specs=[smem, vmem, hbm, vmem],
        out_specs=(hbm, hbm, hbm, hbm, vmem, smem),
        scratch_shapes=[
            pltpu.VMEM((N, 2, 32, width), F32),
            pltpu.VMEM((N, 2, 64, width), F32),
            pltpu.VMEM((N, 32, 128), F32),
            pltpu.VMEM((N, 32, 128), F32),
            pltpu.VMEM((2, fx, width), F32),
            pltpu.VMEM((N, 64, 128), F32),
            pltpu.VMEM((4, 2, 32, 128), F32),
            pltpu.VMEM((4, 2, 32, 128), F32),
            pltpu.VMEM((2, 64, 128), F32),
            pltpu.VMEM((2 * fx, width), BF16),
            pltpu.VMEM((2 * fx, width), BF16),
            pltpu.VMEM((2 * COLS, width), BF16),
            pltpu.VMEM((2 * COLS, width), BF16),
            pltpu.VMEM((2, width, width), BF16),
            pltpu.VMEM((2, width, width), BF16),
            pltpu.VMEM((2 * fx, width), BF16),
            pltpu.VMEM((2 * fx, width), BF16),
            pltpu.VMEM((2 * COLS, width), BF16),
            pltpu.VMEM((2 * COLS, width), BF16),
            pltpu.VMEM((BLOCKS, 2 * fx, 128), F32),
            pltpu.VMEM((BLOCKS, 2 * COLS, 128), F32),
            pltpu.VMEM((4, 2 * fx, 128), F32),
            pltpu.VMEM((4, 2 * COLS, 128), F32),
            dma((2, 2, H)), dma((2, 2, H)), dma((2, 2, H)), dma((2, 2, H)),
            dma((N,)), dma((N,)), dma((6,)), dma((6,)), dma((4,)), dma((4,)), dma((BLOCKS + 1,)), dma,
        ],
        compiler_params=pltpu.CompilerParams(collective_id=0, has_side_effects=True, vmem_limit_bytes=56 * 2**20),
    )(face_blocks, pt, et, maps)

    schur, ext, mult = pl.pallas_call(
        place,
        in_specs=[smem] + [hbm] * 5,
        out_specs=(hbm,) * 3,
        out_shape=(
            jax.ShapeDtypeStruct((2, COLS, 512), F32),
            jax.ShapeDtypeStruct((2, fx, 512), F32),
            jax.ShapeDtypeStruct((2, 64, width), F32),
        ),
        scratch_shapes=[
            pltpu.VMEM((4, 2 * fx, 128), F32),
            pltpu.VMEM((4, 2 * COLS, 128), F32),
            pltpu.VMEM((4, 2 * fx, 128), F32),
            pltpu.VMEM((4, 2 * COLS, 128), F32),
            pltpu.VMEM((2, 64, width), F32),
            pltpu.VMEM((2, COLS, 512), F32),
            pltpu.VMEM((2, fx, 512), F32),
            dma((4, 9)),
        ],
    )(tab, ue, ub, re, rb, mult)
    return jnp.swapaxes(schur, 1, 2), jnp.swapaxes(ext, 1, 2), mult


def solution(mesh):
    in_specs = (P("sib", "box", "grp", None), P("sib", "box", None, "grp"), P("box", "sib", "grp"), P("box", None))
    out_specs = (P("box", "sib", "grp"), P("box", "sib", "grp"), P("box", "grp", "sib"))
    return jax.shard_map(per_device, mesh=mesh, in_specs=in_specs, out_specs=out_specs, check_vma=False)
```

```python
import functools

import jax
import jax.numpy as jnp
from jax import lax
from jax.experimental import pallas as pl
from jax.experimental.pallas import tpu as pltpu
from jax.sharding import PartitionSpec as P

F32, BF16 = jnp.float32, jnp.bfloat16
NN = (((1,), (0,)), ((), ()))
NT = (((1,), (1,)), ((), ()))
MESH = pl.DeviceIdType.MESH
R, L = 0, 1
N = 16
H = N // 2
BLOCKS = 8
COLS = 64


def split(x):
    high = x.astype(BF16)
    return high, (x - high.astype(F32)).astype(BF16)


def dot3(a, b, dims):
    d = functools.partial(lax.dot_general, dimension_numbers=dims, preferred_element_type=F32)
    return d(a[0], b[0]) + d(a[0], b[1]) + d(a[1], b[0])


def combine(z):
    half = z.shape[0] // 2
    a, b = z[:, 0:128], z[:, 128:256]
    return jnp.concatenate([a[0:half] - b[half:], a[half:] + b[0:half]], axis=0)


def look_up(keys, values, key):
    found = jnp.int32(0)
    for k, v in zip(keys, values):
        found = found + jnp.where(k == key, v, 0)
    return found


def tables(faces_ref, s, g, order):
    alpha_order = [faces_ref[0, j] for j in range(BLOCKS)]
    beta_order = [faces_ref[1, j] for j in range(BLOCKS)]
    send = [jnp.int32(0)] * 4
    out, into = jnp.int32(0), jnp.int32(0)
    rank_in = []
    for block in order:
        place = look_up(alpha_order, beta_order, block)
        leaves = jnp.where(place >= 4, 1, 0) != s
        for q in range(4):
            send[q] = send[q] + jnp.where(jnp.logical_and(leaves, out == q), block, 0)
        rank_in.append(jnp.where(leaves, 0, into))
        out = out + jnp.where(leaves, 1, 0)
        into = into + jnp.where(leaves, 0, 1)
    own = [look_up(beta_order, alpha_order, 4 * s + p) for p in range(4)]
    slots = [look_up(order, rank_in, block) for block in own]
    mine = 2 * look_up(beta_order, alpha_order, lax.div(g, 2)) + lax.rem(g, 2)
    panel = [look_up(alpha_order, beta_order, 4 * s + b) for b in range(4)]
    other_panel = [look_up(alpha_order, beta_order, 4 * (1 - s) + b) for b in range(4)]
    return send, own, slots, mine, panel, other_panel


def kernel(
    faces_ref, pt_ref, et_ref, maps_ref,
    ue_out, ub_out, re_out, rb_out, mult_ref, tab_ref,
    pt_all, al_all, pack, held, et_in, maps_in, beta, bsend, brecv, bfull, vh, vl, bvh, bvl, ph, plo, th, tl, bth, btl, ubuf, bbuf, sbuf, sbeta,
    pss, prs, ass, ars, bss, brs, yss, yrs, uss, urs, oss, ess,
):
    s = lax.axis_index("sib")
    g = lax.axis_index("grp")
    other = 1 - s
    width = pt_ref.shape[2]
    fx = et_ref.shape[1]
    width2 = pl.ds(width, width)

    def near(d):
        return lax.rem(g + d + N, N)

    barrier = pltpu.get_barrier_semaphore()
    for peer in ({"grp": near(1)}, {"grp": near(-1)}, {"sib": other}):
        pl.semaphore_signal(barrier, inc=1, device_id=peer, device_id_type=MESH)
    fetch = pltpu.make_async_copy(et_ref, et_in, ess.at[0])
    fetch_pivot = pltpu.make_async_copy(pt_ref, pt_all.at[g], ess.at[1])
    fetch_maps = pltpu.make_async_copy(maps_ref, maps_in, ess.at[2])
    fetch_alpha = pltpu.make_async_copy(maps_ref.at[:, :, pl.ds(0, width)], al_all.at[g], ess.at[3])
    fetch_pivot.start()
    fetch_maps.start()

    @pl.when(s == 0)
    def _():
        fetch_alpha.start()

    fetch.start()
    fetch_maps.wait()

    @pl.when(s == 0)
    def _():
        fetch_alpha.wait()

    @pl.when(s == 1)
    def _():
        lane = lax.broadcasted_iota(jnp.int32, (32, 128), 1)
        for ref, at in ((pack, 0), (held, 32)):
            for t in range(H):
                re = maps_in[0, at : at + 32, t * 128 : (t + 1) * 128]
                im = maps_in[1, at : at + 32, t * 128 : (t + 1) * 128]
                ref[2 * t] = jnp.where(lane < 64, re, pltpu.roll(im, 64, 1))
                ref[2 * t + 1] = jnp.where(lane < 64, pltpu.roll(re, 64, 1), im)

    fetch_pivot.wait()
    pl.semaphore_wait(barrier, 3)

    def hop(buf, ss, rs, way, k, c, arriving):
        back = k if arriving else k - 1
        shard = near(-back if way == R else back)
        return pltpu.make_async_remote_copy(
            src_ref=buf.at[shard, c], dst_ref=buf.at[shard, c],
            send_sem=ss.at[way, c, k - 1], recv_sem=rs.at[way, c, k - 1],
            device_id={"grp": near(1 if way == R else -1)}, device_id_type=MESH,
        )

    def parts(k):
        for c in range(2):
            for way in (R, L):
                if k < H or way == c:
                    yield way, c

    pivot = (pt_all, pss, prs)
    alpha = (al_all, ass, ars)

    def start(ring, k):
        for way, c in parts(k):
            hop(*ring, way, k, c, False).start()

    def forward(ring, k, planes=(0, 1)):
        onward = tuple(parts(k))
        for way, c in parts(k - 1):
            if c not in planes:
                continue
            hop(*ring, way, k - 1, c, True).wait_recv()
            if (way, c) in onward:
                hop(*ring, way, k, c, False).start()

    def arrive(ring, k):
        for way, c in parts(k):
            hop(*ring, way, k, c, True).wait_recv()

    def to_sibling(src, dst, send_sem, recv_sem):
        return pltpu.make_async_remote_copy(
            src_ref=src, dst_ref=dst, send_sem=send_sem, recv_sem=recv_sem, device_id={"sib": other}, device_id_type=MESH
        )

    start(pivot, 1)
    alpha_over = [to_sibling(maps_in.at[c, :, width2], al_all.at[g, c], yss.at[4 + c], yrs.at[4 + c]) for c in range(2)]
    beta_over = to_sibling(pack, held, yss.at[1], yrs.at[1])
    panel_over = to_sibling(bsend, brecv, yss.at[2], yrs.at[2])
    rest_over = to_sibling(sbeta, rb_out, yss.at[3], yrs.at[3])

    @pl.when(s == 0)
    def _():
        for copy in alpha_over:
            copy.start()
        start(alpha, 1)

    @pl.when(s == 1)
    def _():
        beta_over.start()

    forward(pivot, 2)

    @pl.when(s == 1)
    def _():
        for c in range(2):
            alpha_over[c].wait_recv()
            for way in (R, L):
                hop(*alpha, way, 1, c, False).start()

    fetch.wait()

    def prepare(c, _):
        at = pl.ds(pl.multiple_of(c * fx, 16), fx)
        high, low = split(et_in[c])
        vh[at, :] = high
        vl[at, :] = low
        return 0

    lax.fori_loop(0, 2, prepare, 0)

    first = lax.div(g, 2)
    sign = 1 - 2 * lax.rem(g, 2)

    def completes(i):
        return lax.rem(first + sign * lax.div(i + 1, 2) * (1 - 2 * lax.rem(i, 2)) + BLOCKS, BLOCKS)

    forward(pivot, 3)
    send, own, slots, mine, panel, other_panel = tables(faces_ref, s, g, [completes(jnp.int32(i)) for i in range(BLOCKS)])
    for p in range(4):
        tab_ref[p] = own[p]
        tab_ref[4 + p] = slots[p]

    half = pl.ds(pl.multiple_of(s * 32, 32), 32)

    def push(d, arriving):
        to, source = (near(d), g) if not arriving else (g, near(-d))
        return pltpu.make_async_remote_copy(
            src_ref=held.at[to], dst_ref=beta.at[source, half, :],
            send_sem=bss.at[d], recv_sem=brs.at[d],
            device_id={"grp": near(d)}, device_id_type=MESH,
        )

    for k in range(4, H + 1):
        forward(alpha, k // 2, (k % 2,))
        forward(pivot, k)
    forward(alpha, 4, (1,))
    arrive(pivot, H)

    for c in range(2):
        def widen(j, _, c=c):
            high, low = split(pt_all[j, c])
            at = pl.ds(pl.multiple_of(j * 32, 32), 32)
            ph[c, at, :] = high
            plo[c, at, :] = low
            return 0

        lax.fori_loop(0, N, widen, 0)

    def form(q, left, high_ref, low_ref):
        at = pl.ds(pl.multiple_of(q * 128, 128), 128)
        right = tuple(jnp.concatenate([p[0, :, at], p[1, :, at]], axis=1) for p in (ph, plo))
        high, low = split(combine(dot3(tuple(ref[...] for ref in left), right, NN)))
        high_ref[:, at] = high
        low_ref[:, at] = low

    def form_exterior(q, _):
        form(q, (vh, vl), th, tl)
        return 0

    def form_beta(q, _):
        form(q, (bvh, bvl), bth, btl)
        return 0

    def rows_of(block):
        a, b = al_all.at[2 * block], al_all.at[2 * block + 1]
        return split(jnp.concatenate([a[0], b[0], a[1], b[1]], axis=0))

    def keep(block):
        return pltpu.make_async_copy(ubuf.at[block], ue_out.at[block], oss.at[block])

    def partial(i, _):
        block = completes(i)
        ubuf[block] = combine(dot3((th[...], tl[...]), rows_of(block), NT))
        keep(block).start()
        return 0

    def partial_beta(block):
        return combine(dot3((bth[...], btl[...]), rows_of(block), NT))

    def slot(q):
        return to_sibling(sbuf.at[q], re_out.at[q], uss.at[q], urs.at[q])

    def ship(q):
        partial(jnp.int32(4 + q), 0)
        sbuf[q] = ubuf[send[q]]
        slot(q).start()

    lax.fori_loop(0, 4, form_exterior, 0)
    forward(alpha, 5)
    lax.fori_loop(0, 4, partial, 0)
    forward(alpha, 6)
    ship(0)
    forward(alpha, 7)
    @pl.when(s == 0)
    def _():
        beta_over.wait_recv()

    for d in range(1, N):
        push(d, False).start()
    beta[g, half, :] = held[g]
    ship(1)
    forward(alpha, 8)
    ship(2)

    for d in range(1, N):
        push(d, True).wait_recv()
    for b in range(4):
        for c in range(2):
            bsend[b, c] = beta[2 * other_panel[b] + c, half, :]
    panel_over.start()
    arrive(alpha, H)
    ship(3)

    left = split(jnp.concatenate([al_all[mine, 0], al_all[mine, 1]], axis=0))
    zr = dot3(left, (ph[0], plo[0]), NT)
    zi = dot3(left, (ph[1], plo[1]), NT)
    mult_ref[0] = zr[0:64] - zi[64:128]
    mult_ref[1] = zi[0:64] + zr[64:128]

    panel_over.wait_recv()
    for b in range(4):
        for c in range(2):
            bfull[c, half, :] = beta[2 * panel[b] + c, half, :]
            bfull[c, pl.ds(pl.multiple_of(other * 32, 32), 32), :] = brecv[b, c]
        high, low = split(bfull[...].reshape(128, 128).T)
        bvh[:, b * 128 : (b + 1) * 128] = high
        bvl[:, b * 128 : (b + 1) * 128] = low
    lax.fori_loop(0, 4, form_beta, 0)
    for q in range(4):
        sbeta[q] = partial_beta(send[q])
    rest_over.start()
    for p in range(4):
        bbuf[p] = partial_beta(own[p])
    keep_beta = pltpu.make_async_copy(bbuf, ub_out, oss.at[BLOCKS])
    keep_beta.start()

    for ring in (pivot, alpha):
        for k in range(1, H + 1):
            for way, c in parts(k):
                hop(*ring, way, k, c, False).wait_send()
    for d in range(1, N):
        push(d, False).wait_send()

    @pl.when(s == 0)
    def _():
        for copy in alpha_over:
            copy.wait_send()

    @pl.when(s == 1)
    def _():
        beta_over.wait_send()

    for block in range(BLOCKS):
        keep(block).wait()
    keep_beta.wait()
    panel_over.wait_send()
    for q in range(4):
        slot(q).wait()
    rest_over.wait()


def place(tab, ue_ref, ub_ref, re_ref, rb_ref, mult_ref, schur_ref, ext_ref, out_ref, ue, ub, re, rb, mult, schur, ext, sems):
    fx = ext_ref.shape[1]
    through = pltpu.make_async_copy(mult_ref, mult, sems.at[0, 8])
    through.start()
    reads, writes = [], []
    for p in range(4):
        own, slot = tab[p], tab[4 + p]
        pairs = ((ue_ref.at[own], ue.at[p]), (re_ref.at[slot], re.at[p]), (ub_ref.at[p], ub.at[p]), (rb_ref.at[slot], rb.at[p]))
        reads.append([pltpu.make_async_copy(a, b, sems.at[p, i]) for i, (a, b) in enumerate(pairs)])
        for copy in reads[p]:
            copy.start()
    col = lax.broadcasted_iota(jnp.int32, (COLS, 128), 0) + lax.axis_index("grp") * COLS
    row = lax.broadcasted_iota(jnp.int32, (COLS, 128), 1) + lax.axis_index("sib") * 512
    for p in range(4):
        at = slice(p * 128, (p + 1) * 128)
        for copy in reads[p]:
            copy.wait()
        ext[0, :, at] = ue[p, 0:fx] + re[p, 0:fx]
        ext[1, :, at] = ue[p, fx:] + re[p, fx:]
        one = jnp.where(row + p * 128 == col, 1.0, 0.0).astype(F32)
        schur[0, :, at] = one - (ub[p, 0:COLS] + rb[p, 0:COLS])
        schur[1, :, at] = -(ub[p, COLS:] + rb[p, COLS:])
        for i, (a, b) in enumerate(((ext, ext_ref), (schur, schur_ref))):
            writes.append(pltpu.make_async_copy(a.at[:, :, at], b.at[:, :, at], sems.at[p, 4 + i]))
            writes[-1].start()
    through.wait()
    writes.append(pltpu.make_async_copy(mult, out_ref, sems.at[1, 8]))
    writes[-1].start()
    for copy in writes:
        copy.wait()


def per_device(interface_maps, pivot_inverses, exterior_coupling, face_blocks):
    maps = interface_maps[0]
    pt = jnp.swapaxes(pivot_inverses[0], 1, 2)
    et = jnp.swapaxes(exterior_coupling, 1, 2)
    width, fx = pt.shape[2], et.shape[1]
    vmem = pl.BlockSpec(memory_space=pltpu.VMEM)
    smem = pl.BlockSpec(memory_space=pltpu.SMEM)
    hbm = pl.BlockSpec(memory_space=pltpu.HBM)
    dma = pltpu.SemaphoreType.DMA
    ue, ub, re, rb, mult, tab = pl.pallas_call(
        kernel,
        out_shape=(
            jax.ShapeDtypeStruct((BLOCKS, 2 * fx, 128), F32),
            jax.ShapeDtypeStruct((4, 2 * COLS, 128), F32),
            jax.ShapeDtypeStruct((4, 2 * fx, 128), F32),
            jax.ShapeDtypeStruct((4, 2 * COLS, 128), F32),
            jax.ShapeDtypeStruct((2, 64, width), F32),
            jax.ShapeDtypeStruct((8,), jnp.int32),
        ),
        in_specs=[smem, hbm, hbm, hbm],
        out_specs=(hbm, hbm, hbm, hbm, vmem, smem),
        scratch_shapes=[
            pltpu.VMEM((N, 2, 32, width), F32),
            pltpu.VMEM((N, 2, 64, width), F32),
            pltpu.VMEM((N, 32, 128), F32),
            pltpu.VMEM((N, 32, 128), F32),
            pltpu.VMEM((2, fx, width), F32),
            pltpu.VMEM((2, 64, 2 * width), F32),
            pltpu.VMEM((N, 64, 128), F32),
            pltpu.VMEM((4, 2, 32, 128), F32),
            pltpu.VMEM((4, 2, 32, 128), F32),
            pltpu.VMEM((2, 64, 128), F32),
            pltpu.VMEM((2 * fx, width), BF16),
            pltpu.VMEM((2 * fx, width), BF16),
            pltpu.VMEM((2 * COLS, width), BF16),
            pltpu.VMEM((2 * COLS, width), BF16),
            pltpu.VMEM((2, width, width), BF16),
            pltpu.VMEM((2, width, width), BF16),
            pltpu.VMEM((2 * fx, width), BF16),
            pltpu.VMEM((2 * fx, width), BF16),
            pltpu.VMEM((2 * COLS, width), BF16),
            pltpu.VMEM((2 * COLS, width), BF16),
            pltpu.VMEM((BLOCKS, 2 * fx, 128), F32),
            pltpu.VMEM((4, 2 * COLS, 128), F32),
            pltpu.VMEM((4, 2 * fx, 128), F32),
            pltpu.VMEM((4, 2 * COLS, 128), F32),
            dma((2, 2, H)), dma((2, 2, H)), dma((2, 2, H)), dma((2, 2, H)),
            dma((N,)), dma((N,)), dma((6,)), dma((6,)), dma((4,)), dma((4,)), dma((BLOCKS + 1,)), dma((4,)),
        ],
        compiler_params=pltpu.CompilerParams(collective_id=0, has_side_effects=True, vmem_limit_bytes=56 * 2**20),
    )(face_blocks, pt, et, maps)

    schur, ext, mult = pl.pallas_call(
        place,
        in_specs=[smem] + [hbm] * 5,
        out_specs=(hbm,) * 3,
        out_shape=(
            jax.ShapeDtypeStruct((2, COLS, 512), F32),
            jax.ShapeDtypeStruct((2, fx, 512), F32),
            jax.ShapeDtypeStruct((2, 64, width), F32),
        ),
        scratch_shapes=[
            pltpu.VMEM((4, 2 * fx, 128), F32),
            pltpu.VMEM((4, 2 * COLS, 128), F32),
            pltpu.VMEM((4, 2 * fx, 128), F32),
            pltpu.VMEM((4, 2 * COLS, 128), F32),
            pltpu.VMEM((2, 64, width), F32),
            pltpu.VMEM((2, COLS, 512), F32),
            pltpu.VMEM((2, fx, 512), F32),
            dma((4, 9)),
        ],
    )(tab, ue, ub, re, rb, mult)
    return jnp.swapaxes(schur, 1, 2), jnp.swapaxes(ext, 1, 2), mult


def solution(mesh):
    in_specs = (P("sib", "box", "grp", None), P("sib", "box", None, "grp"), P("box", "sib", "grp"), P("box", None))
    out_specs = (P("box", "sib", "grp"), P("box", "sib", "grp"), P("box", "grp", "sib"))
    return jax.shard_map(per_device, mesh=mesh, in_specs=in_specs, out_specs=out_specs, check_vma=False)
```

```python
import functools

import jax
import jax.numpy as jnp
from jax import lax
from jax.experimental import pallas as pl
from jax.experimental.pallas import tpu as pltpu
from jax.sharding import PartitionSpec as P

F32, BF16 = jnp.float32, jnp.bfloat16
NN = (((1,), (0,)), ((), ()))
NT = (((1,), (1,)), ((), ()))
MESH = pl.DeviceIdType.MESH
R, L = 0, 1
N = 16
H = N // 2
BLOCKS = 8
COLS = 64


def split(x):
    high = x.astype(BF16)
    return high, (x - high.astype(F32)).astype(BF16)


def dot3(a, b, dims):
    d = functools.partial(lax.dot_general, dimension_numbers=dims, preferred_element_type=F32)
    return d(a[0], b[0]) + d(a[0], b[1]) + d(a[1], b[0])


def combine(z):
    half = z.shape[0] // 2
    a, b = z[:, 0:128], z[:, 128:256]
    return jnp.concatenate([a[0:half] - b[half:], a[half:] + b[0:half]], axis=0)


def look_up(keys, values, key):
    found = jnp.int32(0)
    for k, v in zip(keys, values):
        found = found + jnp.where(k == key, v, 0)
    return found


def tables(faces_ref, s, g, order):
    alpha_order = [faces_ref[0, j] for j in range(BLOCKS)]
    beta_order = [faces_ref[1, j] for j in range(BLOCKS)]
    send = [jnp.int32(0)] * 4
    out, into = jnp.int32(0), jnp.int32(0)
    rank_in = []
    for block in order:
        place = look_up(alpha_order, beta_order, block)
        leaves = jnp.where(place >= 4, 1, 0) != s
        for q in range(4):
            send[q] = send[q] + jnp.where(jnp.logical_and(leaves, out == q), block, 0)
        rank_in.append(jnp.where(leaves, 0, into))
        out = out + jnp.where(leaves, 1, 0)
        into = into + jnp.where(leaves, 0, 1)
    own = [look_up(beta_order, alpha_order, 4 * s + p) for p in range(4)]
    slots = [look_up(order, rank_in, block) for block in own]
    mine = 2 * look_up(beta_order, alpha_order, lax.div(g, 2)) + lax.rem(g, 2)
    panel = [look_up(alpha_order, beta_order, 4 * s + b) for b in range(4)]
    other_panel = [look_up(alpha_order, beta_order, 4 * (1 - s) + b) for b in range(4)]
    return send, own, slots, mine, panel, other_panel


def kernel(
    faces_ref, pt_ref, et_ref, maps_ref,
    ue_out, ub_out, re_out, rb_out, mult_ref, tab_ref,
    pt_all, al_all, pack, held, et_in, maps_in, beta, bsend, brecv, bfull, vh, vl, bvh, bvl, ph, plo, th, tl, bth, btl, ubuf, bbuf, sbuf, sbeta,
    pss, prs, ass, ars, bss, brs, yss, yrs, uss, urs, oss, ess,
):
    s = lax.axis_index("sib")
    g = lax.axis_index("grp")
    other = 1 - s
    width = pt_ref.shape[2]
    fx = et_ref.shape[1]
    width2 = pl.ds(width, width)

    def near(d):
        return lax.rem(g + d + N, N)

    barrier = pltpu.get_barrier_semaphore()
    for peer in ({"grp": near(1)}, {"grp": near(-1)}, {"sib": other}):
        pl.semaphore_signal(barrier, inc=1, device_id=peer, device_id_type=MESH)
    fetch = pltpu.make_async_copy(et_ref, et_in, ess.at[0])
    fetch_pivot = pltpu.make_async_copy(pt_ref, pt_all.at[g], ess.at[1])
    fetch_maps = pltpu.make_async_copy(maps_ref, maps_in, ess.at[2])
    fetch_alpha = pltpu.make_async_copy(maps_ref.at[:, :, pl.ds(0, width)], al_all.at[g], ess.at[3])
    fetch_pivot.start()
    fetch_maps.start()

    @pl.when(s == 0)
    def _():
        fetch_alpha.start()

    fetch.start()
    fetch_maps.wait()

    @pl.when(s == 0)
    def _():
        fetch_alpha.wait()

    @pl.when(s == 1)
    def _():
        lane = lax.broadcasted_iota(jnp.int32, (32, 128), 1)
        for ref, at in ((pack, 0), (held, 32)):
            for t in range(H):
                re = maps_in[0, at : at + 32, t * 128 : (t + 1) * 128]
                im = maps_in[1, at : at + 32, t * 128 : (t + 1) * 128]
                ref[2 * t] = jnp.where(lane < 64, re, pltpu.roll(im, 64, 1))
                ref[2 * t + 1] = jnp.where(lane < 64, pltpu.roll(re, 64, 1), im)

    fetch_pivot.wait()
    pl.semaphore_wait(barrier, 3)

    def hop(buf, ss, rs, way, k, c, arriving):
        back = k if arriving else k - 1
        shard = near(-back if way == R else back)
        return pltpu.make_async_remote_copy(
            src_ref=buf.at[shard, c], dst_ref=buf.at[shard, c],
            send_sem=ss.at[way, c, k - 1], recv_sem=rs.at[way, c, k - 1],
            device_id={"grp": near(1 if way == R else -1)}, device_id_type=MESH,
        )

    def parts(k):
        for c in range(2):
            for way in (R, L):
                if k < H or way == c:
                    yield way, c

    pivot = (pt_all, pss, prs)
    alpha = (al_all, ass, ars)

    def start(ring, k):
        for way, c in parts(k):
            hop(*ring, way, k, c, False).start()

    def forward(ring, k, planes=(0, 1)):
        onward = tuple(parts(k))
        for way, c in parts(k - 1):
            if c not in planes:
                continue
            hop(*ring, way, k - 1, c, True).wait_recv()
            if (way, c) in onward:
                hop(*ring, way, k, c, False).start()

    def arrive(ring, k):
        for way, c in parts(k):
            hop(*ring, way, k, c, True).wait_recv()

    def to_sibling(src, dst, send_sem, recv_sem):
        return pltpu.make_async_remote_copy(
            src_ref=src, dst_ref=dst, send_sem=send_sem, recv_sem=recv_sem, device_id={"sib": other}, device_id_type=MESH
        )

    start(pivot, 1)
    alpha_over = [to_sibling(maps_in.at[c, :, width2], al_all.at[g, c], yss.at[4 + c], yrs.at[4 + c]) for c in range(2)]
    beta_over = to_sibling(pack, held, yss.at[1], yrs.at[1])
    panel_over = to_sibling(bsend, brecv, yss.at[2], yrs.at[2])
    rest_over = [to_sibling(sbeta.at[q], rb_out.at[q], yss.at[6 + q], yrs.at[6 + q]) for q in range(4)]

    @pl.when(s == 0)
    def _():
        for copy in alpha_over:
            copy.start()
        start(alpha, 1)

    @pl.when(s == 1)
    def _():
        beta_over.start()

    forward(pivot, 2)

    @pl.when(s == 1)
    def _():
        for c in range(2):
            alpha_over[c].wait_recv()
            for way in (R, L):
                hop(*alpha, way, 1, c, False).start()

    fetch.wait()

    def prepare(c, _):
        at = pl.ds(pl.multiple_of(c * fx, 16), fx)
        high, low = split(et_in[c])
        vh[at, :] = high
        vl[at, :] = low
        return 0

    lax.fori_loop(0, 2, prepare, 0)

    first = lax.div(g, 2)
    sign = 1 - 2 * lax.rem(g, 2)

    def completes(i):
        return lax.rem(first + sign * lax.div(i + 1, 2) * (1 - 2 * lax.rem(i, 2)) + BLOCKS, BLOCKS)

    forward(pivot, 3)
    send, own, slots, mine, panel, other_panel = tables(faces_ref, s, g, [completes(jnp.int32(i)) for i in range(BLOCKS)])
    for p in range(4):
        tab_ref[p] = own[p]
        tab_ref[4 + p] = slots[p]

    half = pl.ds(pl.multiple_of(s * 32, 32), 32)

    def push(d, arriving):
        to, source = (near(d), g) if not arriving else (g, near(-d))
        return pltpu.make_async_remote_copy(
            src_ref=held.at[to], dst_ref=beta.at[source, half, :],
            send_sem=bss.at[d], recv_sem=brs.at[d],
            device_id={"grp": near(d)}, device_id_type=MESH,
        )

    for k in range(4, H + 1):
        forward(alpha, k // 2, (k % 2,))
        forward(pivot, k)
    forward(alpha, 4, (1,))
    arrive(pivot, H)

    for c in range(2):
        def widen(j, _, c=c):
            high, low = split(pt_all[j, c])
            at = pl.ds(pl.multiple_of(j * 32, 32), 32)
            ph[c, at, :] = high
            plo[c, at, :] = low
            return 0

        lax.fori_loop(0, N, widen, 0)

    def form(q, left, high_ref, low_ref):
        at = pl.ds(pl.multiple_of(q * 128, 128), 128)
        right = tuple(jnp.concatenate([p[0, :, at], p[1, :, at]], axis=1) for p in (ph, plo))
        high, low = split(combine(dot3(tuple(ref[...] for ref in left), right, NN)))
        high_ref[:, at] = high
        low_ref[:, at] = low

    def form_exterior(q, _):
        form(q, (vh, vl), th, tl)
        return 0

    def form_beta(q, _):
        form(q, (bvh, bvl), bth, btl)
        return 0

    def rows_of(block):
        a, b = al_all.at[2 * block], al_all.at[2 * block + 1]
        return split(jnp.concatenate([a[0], b[0], a[1], b[1]], axis=0))

    def keep(block):
        return pltpu.make_async_copy(ubuf.at[block], ue_out.at[block], oss.at[block])

    def partial(i, _):
        block = completes(i)
        ubuf[block] = combine(dot3((th[...], tl[...]), rows_of(block), NT))
        keep(block).start()
        return 0

    def partial_beta(block):
        return combine(dot3((bth[...], btl[...]), rows_of(block), NT))

    def slot(q):
        return to_sibling(sbuf.at[q], re_out.at[q], uss.at[q], urs.at[q])

    def ship(q):
        partial(jnp.int32(4 + q), 0)
        sbuf[q] = ubuf[send[q]]
        slot(q).start()

    lax.fori_loop(0, 4, form_exterior, 0)
    forward(alpha, 5)
    lax.fori_loop(0, 4, partial, 0)
    forward(alpha, 6)
    ship(0)
    forward(alpha, 7)
    @pl.when(s == 0)
    def _():
        beta_over.wait_recv()

    for d in range(1, N):
        push(d, False).start()
    beta[g, half, :] = held[g]
    ship(1)
    forward(alpha, 8)
    ship(2)

    for d in range(1, N):
        push(d, True).wait_recv()
    for b in range(4):
        for c in range(2):
            bsend[b, c] = beta[2 * other_panel[b] + c, half, :]
    panel_over.start()
    arrive(alpha, H)
    ship(3)

    left = split(jnp.concatenate([al_all[mine, 0], al_all[mine, 1]], axis=0))
    zr = dot3(left, (ph[0], plo[0]), NT)
    zi = dot3(left, (ph[1], plo[1]), NT)
    mult_ref[0] = zr[0:64] - zi[64:128]
    mult_ref[1] = zi[0:64] + zr[64:128]

    panel_over.wait_recv()
    for b in range(4):
        for c in range(2):
            bfull[c, half, :] = beta[2 * panel[b] + c, half, :]
            bfull[c, pl.ds(pl.multiple_of(other * 32, 32), 32), :] = brecv[b, c]
        high, low = split(bfull[...].reshape(128, 128).T)
        bvh[:, b * 128 : (b + 1) * 128] = high
        bvl[:, b * 128 : (b + 1) * 128] = low
    lax.fori_loop(0, 4, form_beta, 0)
    for q in range(4):
        sbeta[q] = partial_beta(send[q])
        rest_over[q].start()
    for p in range(4):
        bbuf[p] = partial_beta(own[p])
    keep_beta = pltpu.make_async_copy(bbuf, ub_out, oss.at[BLOCKS])
    keep_beta.start()

    for ring in (pivot, alpha):
        for k in range(1, H + 1):
            for way, c in parts(k):
                hop(*ring, way, k, c, False).wait_send()
    for d in range(1, N):
        push(d, False).wait_send()

    @pl.when(s == 0)
    def _():
        for copy in alpha_over:
            copy.wait_send()

    @pl.when(s == 1)
    def _():
        beta_over.wait_send()

    for block in range(BLOCKS):
        keep(block).wait()
    keep_beta.wait()
    panel_over.wait_send()
    for q in range(4):
        slot(q).wait()
        rest_over[q].wait()


def place(tab, ue_ref, ub_ref, re_ref, rb_ref, mult_ref, schur_ref, ext_ref, out_ref, ue, ub, re, rb, mult, schur, ext, sems):
    fx = ext_ref.shape[1]
    through = pltpu.make_async_copy(mult_ref, mult, sems.at[0, 8])
    through.start()
    reads, writes = [], []
    for p in range(4):
        own, slot = tab[p], tab[4 + p]
        pairs = ((ue_ref.at[own], ue.at[p]), (re_ref.at[slot], re.at[p]), (ub_ref.at[p], ub.at[p]), (rb_ref.at[slot], rb.at[p]))
        reads.append([pltpu.make_async_copy(a, b, sems.at[p, i]) for i, (a, b) in enumerate(pairs)])
        for copy in reads[p]:
            copy.start()
    col = lax.broadcasted_iota(jnp.int32, (COLS, 128), 0) + lax.axis_index("grp") * COLS
    row = lax.broadcasted_iota(jnp.int32, (COLS, 128), 1) + lax.axis_index("sib") * 512
    for p in range(4):
        at = slice(p * 128, (p + 1) * 128)
        for copy in reads[p]:
            copy.wait()
        ext[0, :, at] = ue[p, 0:fx] + re[p, 0:fx]
        ext[1, :, at] = ue[p, fx:] + re[p, fx:]
        one = jnp.where(row + p * 128 == col, 1.0, 0.0).astype(F32)
        schur[0, :, at] = one - (ub[p, 0:COLS] + rb[p, 0:COLS])
        schur[1, :, at] = -(ub[p, COLS:] + rb[p, COLS:])
        for i, (a, b) in enumerate(((ext, ext_ref), (schur, schur_ref))):
            writes.append(pltpu.make_async_copy(a.at[:, :, at], b.at[:, :, at], sems.at[p, 4 + i]))
            writes[-1].start()
    through.wait()
    writes.append(pltpu.make_async_copy(mult, out_ref, sems.at[1, 8]))
    writes[-1].start()
    for copy in writes:
        copy.wait()


def per_device(interface_maps, pivot_inverses, exterior_coupling, face_blocks):
    maps = interface_maps[0]
    pt = jnp.swapaxes(pivot_inverses[0], 1, 2)
    et = jnp.swapaxes(exterior_coupling, 1, 2)
    width, fx = pt.shape[2], et.shape[1]
    vmem = pl.BlockSpec(memory_space=pltpu.VMEM)
    smem = pl.BlockSpec(memory_space=pltpu.SMEM)
    hbm = pl.BlockSpec(memory_space=pltpu.HBM)
    dma = pltpu.SemaphoreType.DMA
    ue, ub, re, rb, mult, tab = pl.pallas_call(
        kernel,
        out_shape=(
            jax.ShapeDtypeStruct((BLOCKS, 2 * fx, 128), F32),
            jax.ShapeDtypeStruct((4, 2 * COLS, 128), F32),
            jax.ShapeDtypeStruct((4, 2 * fx, 128), F32),
            jax.ShapeDtypeStruct((4, 2 * COLS, 128), F32),
            jax.ShapeDtypeStruct((2, 64, width), F32),
            jax.ShapeDtypeStruct((8,), jnp.int32),
        ),
        in_specs=[smem, hbm, hbm, hbm],
        out_specs=(hbm, hbm, hbm, hbm, vmem, smem),
        scratch_shapes=[
            pltpu.VMEM((N, 2, 32, width), F32),
            pltpu.VMEM((N, 2, 64, width), F32),
            pltpu.VMEM((N, 32, 128), F32),
            pltpu.VMEM((N, 32, 128), F32),
            pltpu.VMEM((2, fx, width), F32),
            pltpu.VMEM((2, 64, 2 * width), F32),
            pltpu.VMEM((N, 64, 128), F32),
            pltpu.VMEM((4, 2, 32, 128), F32),
            pltpu.VMEM((4, 2, 32, 128), F32),
            pltpu.VMEM((2, 64, 128), F32),
            pltpu.VMEM((2 * fx, width), BF16),
            pltpu.VMEM((2 * fx, width), BF16),
            pltpu.VMEM((2 * COLS, width), BF16),
            pltpu.VMEM((2 * COLS, width), BF16),
            pltpu.VMEM((2, width, width), BF16),
            pltpu.VMEM((2, width, width), BF16),
            pltpu.VMEM((2 * fx, width), BF16),
            pltpu.VMEM((2 * fx, width), BF16),
            pltpu.VMEM((2 * COLS, width), BF16),
            pltpu.VMEM((2 * COLS, width), BF16),
            pltpu.VMEM((BLOCKS, 2 * fx, 128), F32),
            pltpu.VMEM((4, 2 * COLS, 128), F32),
            pltpu.VMEM((4, 2 * fx, 128), F32),
            pltpu.VMEM((4, 2 * COLS, 128), F32),
            dma((2, 2, H)), dma((2, 2, H)), dma((2, 2, H)), dma((2, 2, H)),
            dma((N,)), dma((N,)), dma((10,)), dma((10,)), dma((4,)), dma((4,)), dma((BLOCKS + 1,)), dma((4,)),
        ],
        compiler_params=pltpu.CompilerParams(collective_id=0, has_side_effects=True, vmem_limit_bytes=56 * 2**20),
    )(face_blocks, pt, et, maps)

    schur, ext, mult = pl.pallas_call(
        place,
        in_specs=[smem] + [hbm] * 5,
        out_specs=(hbm,) * 3,
        out_shape=(
            jax.ShapeDtypeStruct((2, COLS, 512), F32),
            jax.ShapeDtypeStruct((2, fx, 512), F32),
            jax.ShapeDtypeStruct((2, 64, width), F32),
        ),
        scratch_shapes=[
            pltpu.VMEM((4, 2 * fx, 128), F32),
            pltpu.VMEM((4, 2 * COLS, 128), F32),
            pltpu.VMEM((4, 2 * fx, 128), F32),
            pltpu.VMEM((4, 2 * COLS, 128), F32),
            pltpu.VMEM((2, 64, width), F32),
            pltpu.VMEM((2, COLS, 512), F32),
            pltpu.VMEM((2, fx, 512), F32),
            dma((4, 9)),
        ],
    )(tab, ue, ub, re, rb, mult)
    return jnp.swapaxes(schur, 1, 2), jnp.swapaxes(ext, 1, 2), mult


def solution(mesh):
    in_specs = (P("sib", "box", "grp", None), P("sib", "box", None, "grp"), P("box", "sib", "grp"), P("box", None))
    out_specs = (P("box", "sib", "grp"), P("box", "sib", "grp"), P("box", "grp", "sib"))
    return jax.shard_map(per_device, mesh=mesh, in_specs=in_specs, out_specs=out_specs, check_vma=False)
```
